32 devices in a mesh: lat: 4 (over x, core), lon: 8 (over z, y).
Axes of the slice: x: 2, y: 2, z: 4, core: 2. Of those that a mesh axis runs over, the one named last changes fastest.
Arguments:
- nodes: bfloat16 [4, 8, 384, 512], P('lat', 'lon'), may hold values from -6 to 6
- edges: bfloat16 [4, 8, 3072, 512], P('lat', 'lon'), may hold values from -6 to 6
- senders: int32 [4, 8, 3072], P('lat', 'lon'), may hold values from 0 to 511, as said below
- receivers: int32 [4, 8, 3072], P('lat', 'lon'), may hold values from 0 to 383
- edge_count: int32 [4, 8], P('lat', 'lon'), may hold values from 1536 to 3072, as said below
- halo_send: int32 [4, 8, 4, 24], P('lat', 'lon'), may hold values from 0 to 383
- long_need: int32 [4, 8, 32, 1], P('lat', 'lon'), may hold values from 0 to 1
- node_cot: bfloat16 [4, 8, 384, 512], P('lat', 'lon'), may hold values from -6 to 6
- edge_cot: bfloat16 [4, 8, 3072, 512], P('lat', 'lon'), may hold values from -6 to 6
- e_w1: bfloat16 [1536, 512], replicated, may hold values from -0.15625 to 0.15625
- e_b1: float32 [512], replicated, may hold values from -3 to 3
- e_w2: bfloat16 [512, 512], replicated, may hold values from -0.25 to 0.25
- e_gain: float32 [512], replicated, may hold values from 0.25 to 1.75
- n_w1: bfloat16 [1024, 512], replicated, may hold values from -0.1875 to 0.1875
- n_b1: float32 [512], replicated, may hold values from -3 to 3
- n_w2: bfloat16 [512, 512], replicated, may hold values from -0.25 to 0.25
- n_gain: float32 [512], replicated, may hold values from 0.25 to 1.75
Outputs:
- new_nodes: bfloat16 [4, 8, 384, 512], P('lat', 'lon')
- new_edges: bfloat16 [4, 8, 3072, 512], P('lat', 'lon')
- node_grad: float32 [4, 8, 384, 512], P('lat', 'lon')
- edge_grad: float32 [4, 8, 3072, 512], P('lat', 'lon')
- e_w1_grad: float32 [1536, 512], P(('lat', 'lon'))
- e_b1_grad: float32 [512], P(('lat', 'lon'))
- e_w2_grad: float32 [512, 512], P(('lat', 'lon'))
- e_gain_grad: float32 [512], P(('lat', 'lon'))
- n_w1_grad: float32 [1024, 512], P(('lat', 'lon'))
- n_b1_grad: float32 [512], P(('lat', 'lon'))
- n_w2_grad: float32 [512, 512], P(('lat', 'lon'))
- n_gain_grad: float32 [512], P(('lat', 'lon'))
The draws below stay inside these ranges and needn't reach their ends.
Inputs may be any that keep to these rules, and one draw needn't show every extreme that they name: `senders`: entries below 384 are a region's own nodes, the next 96 the four neighbour blocks, the rest the coarse rows; the third block is never named in the first band and the fourth never in the last. The first three edge slots of region r name the coarse rows of regions r + 1, r - 1 and r + 16 in flat order, counted round. `edge_count`: some region has all 3072 slots live. `long_need`: A region's coarse nodes are its first 2 rows.
All inputs are finite; a program needn't handle non-finite values.
Results may differ from the reference program's by a relative error of at most 0.009.
Values may be sent and summed in bfloat16 or wider, within the bound.
A program may use at most 192 MiB of HBM per device.

```python
import jax
import jax.numpy as jnp
from jax import lax

D = 512
H = 512
NODE_DEV = 384
HALO = 24
COARSE = 2
LONG_SLOT = 1
E_DEV = 3072
N_LAT = 4
N_LON = 8
DEVICES = 32


def draw_senders(key, part):
    keys = jax.random.split(jax.random.fold_in(key, 11), 5)
    shape = (N_LAT, N_LON, E_DEV)
    regions = N_LAT * N_LON
    kind = jax.random.randint(keys[0], shape, 0, 100)
    local = jax.random.randint(keys[1], shape, 0, NODE_DEV)
    block = jax.random.randint(keys[2], shape, 0, 4)
    band = jnp.arange(N_LAT).reshape(N_LAT, 1, 1)
    block = jnp.where((block == 2) & (band == 0), 0, block)
    block = jnp.where((block == 3) & (band == N_LAT - 1), 1, block)
    halo = NODE_DEV + block * HALO + jax.random.randint(keys[3], shape, 0, HALO)
    far = NODE_DEV + 4 * HALO + jax.random.randint(keys[4], shape, 0, regions * LONG_SLOT)
    picked = jnp.where(kind < 80, local, jnp.where(kind < 97, halo, far))
    flat_index = jnp.arange(regions, dtype=jnp.int32).reshape(N_LAT, N_LON, 1)
    offsets = jnp.array([1, regions - 1, regions // 2], dtype=jnp.int32).reshape(1, 1, 3)
    source = (flat_index + offsets) % regions
    fixed_rows = NODE_DEV + 4 * HALO + source * LONG_SLOT
    slot = jnp.arange(E_DEV, dtype=jnp.int32).reshape(1, 1, E_DEV)
    padded = jnp.concatenate([fixed_rows, jnp.zeros((N_LAT, N_LON, E_DEV - 3), jnp.int32)], axis=2)
    return jnp.where(slot < 3, padded, picked).astype(jnp.int32)


def draw_edge_count(key, part):
    keys = jax.random.split(jax.random.fold_in(key, 23), 2)
    counts = jax.random.randint(keys[0], (N_LAT * N_LON,), E_DEV // 2, E_DEV + 1)
    fullest = jax.random.randint(keys[1], (), 0, N_LAT * N_LON)
    counts = jnp.where(jnp.arange(N_LAT * N_LON) == fullest, E_DEV, counts)
    return counts.reshape(N_LAT, N_LON).astype(jnp.int32)


def touch_ends(values, rng, least, top_value):
    longest = values.shape.index(max(values.shape))
    spots = []
    for shift in (0, 1):
        where = [jax.random.randint(jax.random.fold_in(rng, axis), (), 0, length) for axis, length in enumerate(values.shape)]
        where[longest] = (where[longest] + shift) % values.shape[longest]
        spots.append(tuple(where))
    return values.at[spots[0]].set(least).at[spots[1]].set(top_value)


def block_levels(own_key, extent, cuts, least, largest):
    level, own = 1.0, jax.random.fold_in(own_key, 6)
    for dim, blocks in cuts:
        steps = jnp.exp(jax.random.uniform(jax.random.fold_in(own, dim), (blocks,), jnp.float32, least / len(cuts), largest / len(cuts)))
        level = level * jnp.repeat(steps, extent[dim] // blocks).reshape([-1 if axis == dim else 1 for axis in range(len(extent))])
    return level


def noise(key, dims, scale, most, cuts=(), kind=jnp.bfloat16):
    values = scale * jax.random.normal(key, dims, jnp.float32)
    if cuts:
        values = values * block_levels(key, dims, cuts, -0.22, 0.18)
    return jnp.clip(values, -most, most).astype(kind)


def setup_inputs(seed: int = 0) -> dict:
    key_of = jax.random.split(jax.random.key(seed), 18)
    nodes = noise(key_of[0], (N_LAT, N_LON, NODE_DEV, D), 1.0, 6.0, ((0, 4), (1, 8)))
    edges = noise(key_of[1], (N_LAT, N_LON, E_DEV, D), 1.0, 6.0, ((0, 4), (1, 8)))
    senders = draw_senders(jax.random.fold_in(key_of[17], 71), 0)
    receivers = touch_ends(jax.random.randint(key_of[3], (N_LAT, N_LON, E_DEV), 0, NODE_DEV), jax.random.fold_in(key_of[3], 1), 0, NODE_DEV - 1).astype(jnp.int32)
    edge_count = draw_edge_count(jax.random.fold_in(key_of[17], 71), 0)
    halo_send = touch_ends(jax.random.randint(key_of[5], (N_LAT, N_LON, 4, HALO), 0, NODE_DEV), jax.random.fold_in(key_of[5], 1), 0, NODE_DEV - 1).astype(jnp.int32)
    long_need = touch_ends(jax.random.randint(key_of[6], (N_LAT, N_LON, DEVICES, LONG_SLOT), 0, COARSE), jax.random.fold_in(key_of[6], 1), 0, COARSE - 1).astype(jnp.int32)
    node_cot = noise(key_of[7], (N_LAT, N_LON, NODE_DEV, D), 1.0, 6.0, ((0, 4), (1, 8)))
    edge_cot = noise(key_of[8], (N_LAT, N_LON, E_DEV, D), 1.0, 6.0, ((0, 4), (1, 8)))
    e_w1 = noise(key_of[9], (3 * D, H), (3 * D) ** -0.5, 0.15625)
    e_b1 = noise(key_of[10], (H,), 0.5, 3.0, (), jnp.float32)
    e_w2 = noise(key_of[11], (H, D), H ** -0.5, 0.25)
    e_gain = jnp.clip(1.0 + 0.15 * jax.random.normal(key_of[12], (D,), jnp.float32), 0.25, 1.75)
    n_w1 = noise(key_of[13], (2 * D, H), (2 * D) ** -0.5, 0.1875)
    n_b1 = noise(key_of[14], (H,), 0.5, 3.0, (), jnp.float32)
    n_w2 = noise(key_of[15], (H, D), H ** -0.5, 0.25)
    n_gain = jnp.clip(1.0 + 0.15 * jax.random.normal(key_of[16], (D,), jnp.float32), 0.25, 1.75)
    return {"nodes": nodes, "edges": edges, "senders": senders, "receivers": receivers, "edge_count": edge_count, "halo_send": halo_send, "long_need": long_need, "node_cot": node_cot, "edge_cot": edge_cot, "e_w1": e_w1, "e_b1": e_b1, "e_w2": e_w2, "e_gain": e_gain, "n_w1": n_w1, "n_b1": n_b1, "n_w2": n_w2, "n_gain": n_gain}


EPS = 1e-05

def layer_norm(z, gain):
    mean = lax.optimization_barrier(jnp.mean(z, axis=-1, keepdims=True))
    centred = z - mean
    rstd = lax.rsqrt(lax.optimization_barrier(jnp.mean(centred * centred, axis=-1, keepdims=True)) + EPS)
    normed = centred * rstd
    return (normed * gain, normed, rstd)

def transposed(left, right):
    return lax.dot_general(left, right, (((0,), (0,)), ((), ())), preferred_element_type=jnp.float32)

def mlp_forward(parts, w_first, b_first, w_second, gain):
    joined = jnp.concatenate(parts, axis=1)
    z_first = jnp.dot(joined, w_first, preferred_element_type=jnp.float32) + b_first
    active = jax.nn.silu(z_first).astype(jnp.bfloat16)
    z_second = jnp.dot(active, w_second, preferred_element_type=jnp.float32)
    result, normed, rstd = layer_norm(z_second, gain)
    return (result, (z_first, active, normed, rstd))

def mlp_backward(parts, saved, grad_out, w_first, w_second, gain):
    z_first, active, normed, rstd = saved
    gain_grad = lax.optimization_barrier(jnp.sum(grad_out * normed, axis=0))
    scaled = grad_out * gain
    g_second = rstd * (scaled - lax.optimization_barrier(jnp.mean(scaled, axis=-1, keepdims=True)) - normed * lax.optimization_barrier(jnp.mean(scaled * normed, axis=-1, keepdims=True)))
    g_second = g_second.astype(jnp.bfloat16)
    second_grad = transposed(active, g_second)
    g_active = jnp.dot(g_second, w_second.T, preferred_element_type=jnp.float32)
    sigma = jax.nn.sigmoid(z_first)
    g_first = (g_active * sigma * (1.0 + z_first * (1.0 - sigma))).astype(jnp.bfloat16)
    bias_grad = lax.optimization_barrier(jnp.sum(g_first, axis=0, dtype=jnp.float32))
    joined = jnp.concatenate(parts, axis=1)
    first_grad = transposed(joined, g_first)
    g_input = jnp.dot(g_first, w_first.T, preferred_element_type=jnp.float32)
    return (g_input, (first_grad, bias_grad, second_grad, gain_grad))

def device_pass(table, nodes_l, edges_l, snd, rcv, count, node_cot_l, edge_cot_l, weights):
    e_w1, e_b1, e_w2, e_gain, n_w1, n_b1, n_w2, n_gain = weights
    width = nodes_l.shape[1]
    node_n = nodes_l.shape[0]
    sent_rows = jnp.take(table, snd, axis=0)
    recv_rows = jnp.take(nodes_l, rcv, axis=0)
    edge_parts = (edges_l, sent_rows, recv_rows)
    edge_out, edge_saved = mlp_forward(edge_parts, e_w1, e_b1, e_w2, e_gain)
    alive = jnp.arange(edges_l.shape[0]) < count
    live = alive.astype(jnp.float32)[:, None]
    new_edges = (edges_l + live * edge_out).astype(jnp.bfloat16)
    recv_table = ((rcv[None, :] == jnp.arange(node_n)[:, None]) & alive[None, :]).astype(jnp.bfloat16)
    aggregate = jnp.dot(recv_table, new_edges, preferred_element_type=jnp.float32).astype(jnp.bfloat16)
    node_parts = (nodes_l, aggregate)
    node_out, node_saved = mlp_forward(node_parts, n_w1, n_b1, n_w2, n_gain)
    new_nodes = (nodes_l + node_out).astype(jnp.bfloat16)
    node_up = node_cot_l.astype(jnp.float32)
    g_node_in, node_grads = mlp_backward(node_parts, node_saved, node_up, n_w1, n_w2, n_gain)
    g_aggregate = g_node_in[:, width:]
    g_new_edges = edge_cot_l.astype(jnp.float32) + live * jnp.take(g_aggregate, rcv, axis=0)
    g_edge_in, edge_grads = mlp_backward(edge_parts, edge_saved, live * g_new_edges, e_w1, e_w2, e_gain)
    g_edge_in = g_edge_in.astype(jnp.bfloat16)
    edge_grad = g_new_edges + g_edge_in[:, :width]
    node_local = node_up + g_node_in[:, :width] + jnp.dot(recv_table, g_edge_in[:, 2 * width:], preferred_element_type=jnp.float32)
    send_table = (snd[None, :] == jnp.arange(table.shape[0])[:, None]).astype(jnp.bfloat16)
    sender_grad = jnp.dot(send_table, g_edge_in[:, width:2 * width], preferred_element_type=jnp.float32)
    return (new_nodes, new_edges, edge_grad, node_local, sender_grad, edge_grads + node_grads)

def pick_rows(source, rows):
    return jnp.take(source, rows, axis=0)

def add_rows(rows, values, node_n, width):
    return jnp.zeros((node_n, width), jnp.float32).at[rows].add(values)

def reference(nodes, edges, senders, receivers, edge_count, halo_send, long_need, node_cot, edge_cot, e_w1, e_b1, e_w2, e_gain, n_w1, n_b1, n_w2, n_gain):
    lat_n, lon_n, node_n, width = nodes.shape
    devices = lat_n * lon_n
    halo_n = halo_send.shape[3]
    slot_n = long_need.shape[3]
    sent = jax.vmap(jax.vmap(pick_rows))(nodes, halo_send)
    zero_band = jnp.zeros_like(sent[:1, :, 2])
    block_east = jnp.roll(sent[:, :, 0], 1, axis=1)
    block_west = jnp.roll(sent[:, :, 1], -1, axis=1)
    block_north = jnp.concatenate([zero_band, sent[:-1, :, 2]], axis=0)
    block_south = jnp.concatenate([sent[1:, :, 3], zero_band], axis=0)
    halo = jnp.stack([block_east, block_west, block_north, block_south], axis=2).reshape(lat_n, lon_n, 4 * halo_n, width)
    coarse = nodes[:, :, :COARSE].reshape(devices * COARSE, width)
    far_ids = (jnp.arange(devices, dtype=jnp.int32)[:, None] * COARSE + long_need).reshape(lat_n, lon_n, devices * slot_n)
    far = jnp.take(coarse, far_ids, axis=0)
    table = jnp.concatenate([nodes, halo, far], axis=2).reshape(devices, -1, width)
    weights = (e_w1, e_b1, e_w2, e_gain, n_w1, n_b1, n_w2, n_gain)

    def flat(array):
        return array.reshape((devices,) + array.shape[2:])
    inputs = (table, flat(nodes), flat(edges), flat(senders), flat(receivers), edge_count.reshape(devices), flat(node_cot), flat(edge_cot))
    init = tuple((jnp.zeros(weight.shape, jnp.float32) for weight in weights))

    def step(carry, item):
        new_nodes, new_edges, edge_grad, node_local, sender_grad, grads = device_pass(*item, weights)
        carry = tuple((total + grad for total, grad in zip(carry, grads)))
        return (carry, (new_nodes, new_edges, edge_grad, node_local, sender_grad))
    sums, outputs = lax.scan(step, init, inputs)
    new_nodes, new_edges, edge_grad, node_local, sender_grad = outputs
    sender_grad = sender_grad.reshape(lat_n, lon_n, -1, width)
    halo_grad = sender_grad[:, :, node_n:node_n + 4 * halo_n].reshape(lat_n, lon_n, 4, halo_n, width)
    far_grad = sender_grad[:, :, node_n + 4 * halo_n:]
    zero_grad = jnp.zeros_like(halo_grad[:1, :, 2])
    back_east = jnp.roll(halo_grad[:, :, 0], -1, axis=1)
    back_west = jnp.roll(halo_grad[:, :, 1], 1, axis=1)
    back_north = jnp.concatenate([halo_grad[1:, :, 2], zero_grad], axis=0)
    back_south = jnp.concatenate([zero_grad, halo_grad[:-1, :, 3]], axis=0)
    back = jnp.stack([back_east, back_west, back_north, back_south], axis=2).reshape(lat_n, lon_n, 4 * halo_n, width)
    node_grad = node_local.reshape(lat_n, lon_n, node_n, width) + sender_grad[:, :, :node_n]
    returned = jax.vmap(jax.vmap(lambda rows, values: add_rows(rows, values, node_n, width)))(halo_send.reshape(lat_n, lon_n, 4 * halo_n), back)
    node_grad = node_grad + returned
    coarse_grad = jax.ops.segment_sum(far_grad.reshape(-1, width), far_ids.reshape(-1), num_segments=devices * COARSE)
    node_grad = node_grad.at[:, :, :COARSE].add(coarse_grad.reshape(lat_n, lon_n, COARSE, width))
    return (new_nodes.reshape(nodes.shape), new_edges.reshape(edges.shape), node_grad, edge_grad.reshape(edges.shape), sums[0], sums[1], sums[2], sums[3], sums[4], sums[5], sums[6], sums[7])
```

```python
import functools

import jax
import jax.numpy as jnp
from jax import lax
from jax.experimental import pallas as pl
from jax.experimental.pallas import tpu as pltpu
from jax.sharding import PartitionSpec as P

COARSE = 2
EPS = 1e-05
LANES = 128
TILE = 512
BF = jnp.bfloat16
F32 = jnp.float32
VMEM = pltpu.VMEM


def dot(a, b):
    return jnp.dot(a, b, preferred_element_type=F32)


def dot_nt(a, b):
    return lax.dot_general(a, b, (((1,), (1,)), ((), ())), preferred_element_type=F32)


def dot_tn(a, b):
    return lax.dot_general(a, b, (((0,), (0,)), ((), ())), preferred_element_type=F32)


def iota(shape, dim):
    return lax.broadcasted_iota(jnp.int32, shape, dim)


def onehot(mask):
    return jnp.where(mask, 1.0, 0.0).astype(BF)


def up(n, m):
    return -(-n // m) * m


class Sizes:
    def __init__(self, mesh, node_n, halo_n, slot_n):
        self.lat, self.lon = mesh.shape["lat"], mesh.shape["lon"]
        self.dev = self.lat * self.lon
        self.node = node_n
        self.halo = halo_n
        self.hslot = up(halo_n, 16)
        self.hrows = up(4 * self.hslot, LANES)
        self.slot = slot_n
        self.far_n = self.dev * slot_n
        self.far = up(self.far_n, LANES)
        self.recv_at = node_n + self.hrows
        self.far_at = self.recv_at + node_n
        self.cols = self.far_at + self.far
        self.core = 2 if self.lat % 2 == 0 else 1
        self.x = self.lat // self.core
        self.y = 2 if self.lon % 2 == 0 else 1
        self.z = self.lon // self.y


def flat_device(s, r):
    return {"lat": r // s.lon, "lon": r % s.lon}


def remote(src, dst, send, recv, peer):
    return pltpu.make_async_remote_copy(
        src_ref=src,
        dst_ref=dst,
        send_sem=send,
        recv_sem=recv,
        device_id=peer,
        device_id_type=pl.DeviceIdType.MESH,
    )


def neighbours(s):
    a, b = lax.axis_index("lat"), lax.axis_index("lon")
    east, west = (b + 1) % s.lon, (b + s.lon - 1) % s.lon
    south, north = (a + 1) % s.lat, (a + s.lat - 1) % s.lat
    return [
        {"lat": a, "lon": east},
        {"lat": a, "lon": west},
        {"lat": south, "lon": b},
        {"lat": north, "lon": b},
    ]


def coarse_rows(s, need, q, width):
    spot = (iota((1, s.far), 1) // s.slot) * (COARSE * width // LANES)
    row = jnp.where(need < 0, -1, spot + need * (width // LANES) + q)
    return onehot(iota((s.dev * COARSE * width // LANES, s.far), 0) == row)


def table_kernel(
    s, nodes, out_rows, need, ext, own, sent, came, far_in, send_h, recv_h, send_c, recv_c
):
    width = nodes.shape[1]
    cuts = width // LANES
    a, b = lax.axis_index("lat"), lax.axis_index("lon")
    me = a * s.lon + b
    barrier = pltpu.get_barrier_semaphore()

    def greet(d, _):
        pl.semaphore_signal(
            barrier, 1, device_id=flat_device(s, (me + d) % s.dev), device_id_type=pl.DeviceIdType.MESH
        )
        return 0

    lax.fori_loop(1, s.dev, greet, 0)
    top = nodes[0:16, :].astype(F32)
    for c in range(COARSE):
        for q in range(cuts):
            j = c * cuts + q
            own[j : j + 1, :] = top[c : c + 1, q * LANES : (q + 1) * LANES]
    pick = onehot(iota((s.node, s.hrows), 0) == out_rows[0:1, :])
    sent[...] = dot_tn(pick, nodes[...]).astype(BF)
    pl.semaphore_wait(barrier, s.dev - 1)
    copies = []
    for k, peer in enumerate(neighbours(s)):
        rows = pl.ds(k * s.hslot, s.hslot)
        copies.append(remote(sent.at[rows], came.at[rows], send_h.at[k], recv_h.at[k], peer))
        copies[-1].start()
    units = COARSE * cuts

    def coarse_copy(d):
        return remote(
            own,
            far_in.at[pl.ds(me * units, units)],
            send_c.at[d],
            recv_c.at[d],
            flat_device(s, (me + d) % s.dev),
        )

    def push(d, _):
        coarse_copy(d).start()
        return 0

    lax.fori_loop(1, s.dev, push, 0)
    far_in[pl.ds(me * units, units), :] = own[...]
    for copy in copies:
        copy.wait()
    block = iota((s.hrows, 1), 0) // s.hslot
    dead = ((block == 2) & (a == 0)) | ((block == 3) & (a == s.lat - 1))
    ext[0 : s.hrows, :] = jnp.where(dead, 0.0, came[...].astype(F32)).astype(BF)

    def settle(d, _):
        coarse_copy(d).wait()
        return 0

    lax.fori_loop(1, s.dev, settle, 0)
    rows = far_in[...].astype(BF)
    for q in range(cuts):
        pick = coarse_rows(s, need[0:1, :], q, width)
        ext[s.hrows :, q * LANES : (q + 1) * LANES] = dot_tn(pick, rows).astype(BF)


def exchange_table(s, nodes, out_rows, need):
    width = nodes.shape[1]
    units = COARSE * width // LANES
    full = pl.BlockSpec(memory_space=VMEM)
    return pl.pallas_call(
        functools.partial(table_kernel, s),
        out_shape=jax.ShapeDtypeStruct((s.hrows + s.far, width), BF),
        in_specs=[full] * 3,
        out_specs=full,
        scratch_shapes=[
            VMEM((units, LANES), F32),
            VMEM((s.hrows, width), BF),
            VMEM((s.hrows, width), BF),
            VMEM((s.dev * units, LANES), F32),
            pltpu.SemaphoreType.DMA((4,)),
            pltpu.SemaphoreType.DMA((4,)),
            pltpu.SemaphoreType.DMA((s.dev,)),
            pltpu.SemaphoreType.DMA((s.dev,)),
        ],
        compiler_params=pltpu.CompilerParams(collective_id=0, has_side_effects=True),
        name="table",
    )(nodes, out_rows, need)


def normalise(z):
    mean = jnp.mean(z, axis=-1, keepdims=True)
    centred = z - mean
    rstd = lax.rsqrt(jnp.mean(centred * centred, axis=-1, keepdims=True) + EPS)
    return centred * rstd, rstd


def gate(z):
    sig = 1.0 / (1.0 + jnp.exp(-z))
    return (z * sig).astype(BF), sig * (1.0 + z * (1.0 - sig))


def norm_back(scaled, normed, rstd):
    return rstd * (
        scaled
        - jnp.mean(scaled, axis=-1, keepdims=True)
        - normed * jnp.mean(scaled * normed, axis=-1, keepdims=True)
    )


def layer_kernel(
    s,
    count,
    snd,
    rcv,
    nodes,
    ext,
    edges,
    edge_cot,
    node_cot,
    e_w1,
    e_b1,
    e_w2,
    e_gain,
    n_w1,
    n_b1,
    n_w2,
    n_gain,
    new_edges,
    edge_grad,
    new_nodes,
    node_part,
    ext_grad,
    early,
    late,
    vectors,
    snd_s,
    rcv_s,
    mix,
    pick,
    pick_t,
    active,
    slope,
    normed,
    rstd,
    agg,
    g_agg,
    spread,
    w_edge_grad,
    w_two_grad,
):
    i = pl.program_id(0)
    width = nodes.shape[1]
    steps = pick.shape[0]
    tile = pick.shape[1]
    groups = tile // LANES
    dev = s.dev

    @pl.when(i == 0)
    def _():
        lives = snd_s.shape[0] * LANES
        place = iota(snd_s.shape, 0) * LANES + iota(snd_s.shape, 1)
        live = place < count[0, 0]
        ids = snd[...]
        base = s.node
        moved = ids
        for k in range(1, 4):
            moved = moved + jnp.where(ids >= base + k * s.halo, s.hslot - s.halo, 0)
        ends = base + 4 * s.halo
        moved = jnp.where(ids >= ends, ids - ends + s.far_at, moved)
        snd_s[...] = jnp.where(live, moved, -1)
        rcv_s[...] = jnp.where(live, rcv[...] + s.recv_at, -1)
        mix[0:width, :] = e_w1[0:width, :]
        w_send, w_recv = e_w1[width : 2 * width, :], e_w1[2 * width :, :]
        at = width
        mix[at : at + s.node, :] = dot(nodes[...], w_send).astype(BF)
        mix[at + s.node : at + s.recv_at, :] = dot(ext[0 : s.hrows, :], w_send).astype(BF)
        mix[at + s.recv_at : at + s.far_at, :] = dot(nodes[...], w_recv).astype(BF)
        mix[at + s.far_at :, :] = dot(ext[s.hrows :, :], w_send).astype(BF)
        agg[...] = jnp.zeros_like(agg)
        spread[...] = jnp.zeros_like(spread)
        w_edge_grad[...] = jnp.zeros_like(w_edge_grad)
        w_two_grad[...] = jnp.zeros_like(w_two_grad)
        vectors[...] = jnp.zeros_like(vectors)

    def rows_of(c):
        return s.recv_at <= c < s.far_at

    @pl.when(i < steps)
    def _():
        live = (iota((tile, 1), 0) + i * tile) < count[0, 0]
        for g in range(groups):
            at = i * groups + g
            srow, rrow = snd_s[pl.ds(at, 1), :], rcv_s[pl.ds(at, 1), :]
            scol = jnp.broadcast_to(srow, (LANES, LANES)).T
            rcol = jnp.broadcast_to(rrow, (LANES, LANES)).T
            lane = iota((LANES, LANES), 1)
            sub = iota((LANES, LANES), 0)
            span = slice(g * LANES, (g + 1) * LANES)
            for c in range(0, s.cols, LANES):
                col, row = (rcol, rrow) if rows_of(c) else (scol, srow)
                pick[i, span, c : c + LANES] = onehot(lane + c == col)
                pick_t[i, c : c + LANES, span] = onehot(sub + c == row)
        e = edges[...]
        z = dot(jnp.concatenate([e, pick[i]], axis=1), mix[...]) + e_b1[...]
        act, back = gate(z)
        active[i] = act
        slope[i] = back.astype(BF)
        unit, scale = normalise(dot(act, e_w2[...]))
        normed[i] = unit.astype(BF)
        rstd[i] = scale
        fresh = (e.astype(F32) + jnp.where(live, unit * e_gain[...], 0.0)).astype(BF)
        new_edges[...] = fresh
        agg[...] += dot(pick_t[i, s.recv_at : s.far_at, :], fresh)

    @pl.when(i == steps - 1)
    def _():
        own = nodes[...]
        both = jnp.concatenate([own, agg[...].astype(BF)], axis=1)
        act, back = gate(dot(both, n_w1[...]) + n_b1[...])
        unit, scale = normalise(dot(act, n_w2[...]))
        new_nodes[...] = (own.astype(F32) + unit * n_gain[...]).astype(BF)
        g = node_cot[...].astype(F32)
        vectors[3:4, :] = jnp.sum(g * unit, axis=0, keepdims=True)
        g_two = norm_back(g * n_gain[...], unit, scale).astype(BF)
        n_two = dot_tn(act, g_two).astype(BF)
        g_one = (dot_nt(g_two, n_w2[...]) * back).astype(BF)
        vectors[2:3, :] = jnp.sum(g_one.astype(F32), axis=0, keepdims=True)
        n_one = dot_tn(both, g_one).astype(BF)
        g_in = dot_nt(g_one, n_w1[...])
        node_part[...] = g + g_in[:, :width]
        g_agg[...] = g_in[:, width:].astype(BF)
        one, two = n_one.shape[0] // dev, n_two.shape[0] // dev
        for d in range(dev):
            early[d, 0:one, :] = n_one[d * one : (d + 1) * one, :]
            early[d, one : one + two, :] = n_two[d * two : (d + 1) * two, :]

    @pl.when(i >= steps)
    def _():
        t = i - steps
        live = (iota((tile, 1), 0) + t * tile) < count[0, 0]
        d_new = edge_cot[...].astype(F32) + dot(pick[t, :, s.recv_at : s.far_at], g_agg[...])
        g = jnp.where(live, d_new, 0.0)
        unit = normed[t].astype(F32)
        vectors[1:2, :] += jnp.sum(g * unit, axis=0, keepdims=True)
        g_two = norm_back(g * e_gain[...], unit, rstd[t]).astype(BF)
        w_two_grad[...] += dot_tn(active[t], g_two)
        g_one = (dot_nt(g_two, e_w2[...]) * slope[t].astype(F32)).astype(BF)
        vectors[0:1, :] += jnp.sum(g_one.astype(F32), axis=0, keepdims=True)
        w_edge_grad[...] += dot_tn(edges[...], g_one)
        spread[...] += dot(pick_t[t], g_one)
        edge_grad[...] = d_new + dot_nt(g_one, e_w1[0:width, :])

    @pl.when(i == 2 * steps - 1)
    def _():
        w_send, w_recv = e_w1[width : 2 * width, :], e_w1[2 * width :, :]
        own = nodes[...]
        s_own = spread[0 : s.node, :].astype(BF)
        s_halo = spread[s.node : s.recv_at, :].astype(BF)
        s_recv = spread[s.recv_at : s.far_at, :].astype(BF)
        s_far = spread[s.far_at :, :].astype(BF)
        late[0:width, :] = w_edge_grad[...].astype(BF)
        late[width : 2 * width, :] = (
            dot_tn(own, s_own) + dot_tn(ext[0 : s.hrows, :], s_halo) + dot_tn(ext[s.hrows :, :], s_far)
        ).astype(BF)
        late[2 * width :, :] = dot_tn(own, s_recv).astype(BF)
        two = w_two_grad.shape[0] // dev
        at = early.shape[1] - two
        for d in range(dev):
            early[d, at:, :] = w_two_grad[d * two : (d + 1) * two, :].astype(BF)
        node_part[...] += dot_nt(s_own, w_send) + dot_nt(s_recv, w_recv)
        ext_grad[0 : s.hrows, :] = dot_nt(s_halo, w_send).astype(BF)
        ext_grad[s.hrows :, :] = dot_nt(s_far, w_send).astype(BF)


def layer(s, count, snd, rcv, nodes, ext, edges, edge_cot, node_cot, weights):
    edge_n, width = edges.shape
    hidden = weights[2].shape[0]
    steps = edge_n // TILE
    whole = pl.BlockSpec(memory_space=VMEM)
    smem = pl.BlockSpec(memory_space=pltpu.SMEM)
    once = functools.partial(pl.BlockSpec, pipeline_mode=pl.Buffered(1))

    def fixed(shape):
        return once(shape, lambda i: (0,) * len(shape))

    def tile(index):
        return pl.BlockSpec((TILE, width), lambda i: (index(i), 0))

    both = tile(lambda i: lax.rem(i, steps))
    first = tile(lambda i: jnp.minimum(i, steps - 1))
    second = tile(lambda i: jnp.maximum(i - steps, 0))
    inputs = (count, snd, rcv, nodes, ext, edges, edge_cot, node_cot) + weights
    in_specs = [smem] + [fixed(v.shape) for v in inputs[1:]]
    in_specs[5], in_specs[6] = both, second
    per = (weights[4].shape[0] + weights[6].shape[0] + weights[2].shape[0]) // s.dev
    late_n = weights[0].shape[0]
    out = [
        ((edge_n, width), BF, first),
        ((edge_n, width), F32, second),
        (nodes.shape, BF, None),
        (nodes.shape, F32, None),
        ((s.hrows + s.far, width), BF, None),
        ((s.dev, per, width), BF, None),
        ((late_n, width), BF, None),
        ((8, width), F32, None),
    ]
    return pl.pallas_call(
        functools.partial(layer_kernel, s),
        grid=(2 * steps,),
        out_shape=[jax.ShapeDtypeStruct(shape, kind) for shape, kind, _ in out],
        in_specs=in_specs,
        out_specs=[spec or fixed(shape) for shape, _, spec in out],
        scratch_shapes=[
            VMEM(snd.shape, jnp.int32),
            VMEM(snd.shape, jnp.int32),
            VMEM((width + s.cols, hidden), BF),
            VMEM((steps, TILE, s.cols), BF),
            VMEM((steps, s.cols, TILE), BF),
            VMEM((steps, TILE, hidden), BF),
            VMEM((steps, TILE, hidden), BF),
            VMEM((steps, TILE, width), BF),
            VMEM((steps, TILE, 1), F32),
            VMEM((s.node, width), F32),
            VMEM((s.node, width), BF),
            VMEM((s.cols, hidden), F32),
            VMEM((width, hidden), F32),
            VMEM((hidden, width), F32),
        ],
        compiler_params=pltpu.CompilerParams(
            dimension_semantics=("arbitrary",), vmem_limit_bytes=63 * 1024 * 1000
        ),
        name="layer",
    )(*inputs)


def reduce_kernel(
    s,
    out_rows,
    need,
    node_part,
    ext_grad,
    early,
    late,
    vectors,
    node_grad,
    early_out,
    late_out,
    vec_out,
    fold,
    back,
    e0,
    l0,
    f0,
    v0,
    e1,
    l1,
    f1,
    v1,
    er1,
    lr1,
    fr1,
    vr1,
    e2,
    l2,
    f2,
    v2,
    er2,
    lr2,
    fr2,
    vr2,
    send_h,
    recv_h,
    send0,
    recv0,
    send1,
    recv1,
    send2,
    recv2,
):
    width = node_part.shape[1]
    cuts = width // LANES
    units = COARSE * cuts
    a, b = lax.axis_index("lat"), lax.axis_index("lon")
    x, core = a // s.core, a % s.core
    z, y = b // s.y, b % s.y
    barrier = pltpu.get_barrier_semaphore()
    around = neighbours(s)
    partner = {"lat": x * s.core + (core + 1) % s.core, "lon": b}
    plane = [(dx, dy) for dx in range(s.x) for dy in range(s.y) if dx or dy]

    def plane_peer(dx, dy):
        return {
            "lat": ((x + dx) % s.x) * s.core + core,
            "lon": z * s.y + (y + dy) % s.y,
        }

    def line_peer(dz):
        return {"lat": a, "lon": ((z + dz) % s.z) * s.y + y}

    peers = around + [partner] + [plane_peer(*p) for p in plane]
    peers = peers + [line_peer(dz) for dz in range(1, s.z)]
    for peer in peers:
        pl.semaphore_signal(barrier, 1, device_id=peer, device_id_type=pl.DeviceIdType.MESH)
    far = ext_grad[s.hrows :, :]
    total = jnp.zeros(fold.shape, F32)
    for q in range(cuts):
        total = total + dot(
            coarse_rows(s, need[0:1, :], q, width), far[:, q * LANES : (q + 1) * LANES]
        )
    fold[...] = total
    pl.semaphore_wait(barrier, len(peers))
    copies = []
    homes = [around[1], around[0], around[3], around[2]]
    for k, peer in enumerate(homes):
        rows = pl.ds(k * s.hslot, s.hslot)
        copies.append(remote(ext_grad.at[rows], back.at[rows], send_h.at[k], recv_h.at[k], peer))
    block = s.z * s.y
    other = (core + 1) % s.core
    stage0 = []
    for xx in range(s.x):
        rows = pl.ds((xx * s.core + other) * block, block)
        stage0.append(remote(early.at[rows], e0.at[xx], send0.at[0, xx], recv0.at[0, xx], partner))
        per = late.shape[0] // s.dev
        stage0.append(remote(late.at[rows], l0.at[xx], send0.at[1, xx], recv0.at[1, xx], partner))
        stage0.append(
            remote(
                fold.at[pl.ds((xx * s.core + other) * block * units, block * units)],
                f0.at[xx],
                send0.at[2, xx],
                recv0.at[2, xx],
                partner,
            )
        )
    stage0.append(remote(vectors, v0, send0.at[3, 0], recv0.at[3, 0], partner))
    for copy in copies + stage0:
        copy.start()
    for copy in stage0:
        copy.wait()
    for xx in range(s.x):
        for zz in range(s.z):
            for yy in range(s.y):
                src = (xx * s.core + core) * block + zz * s.y + yy
                pos = zz * s.y + yy
                to = xx * s.y + yy
                e1[to, zz] = (early[src].astype(F32) + e0[xx, pos].astype(F32)).astype(BF)
                l1[to, zz] = (late[src].astype(F32) + l0[xx, pos].astype(F32)).astype(BF)
                f1[to, pl.ds(zz * units, units)] = (
                    fold[pl.ds(src * units, units), :] + f0[xx, pl.ds(pos * units, units)]
                )
    v1[...] = vectors[...] + v0[...]
    stage1 = []
    for n, (dx, dy) in enumerate(plane):
        to = ((x + dx) % s.x) * s.y + (y + dy) % s.y
        peer = plane_peer(dx, dy)
        for k, (src, dst) in enumerate(((e1, er1), (l1, lr1), (f1, fr1))):
            stage1.append(remote(src.at[to], dst.at[n], send1.at[k, n], recv1.at[k, n], peer))
        stage1.append(remote(v1, vr1.at[n], send1.at[3, n], recv1.at[3, n], peer))
    for copy in stage1:
        copy.start()
    for copy in stage1:
        copy.wait()
    mine = x * s.y + y
    e_sum, l_sum = e1[mine].astype(F32), l1[mine].astype(F32)
    f_sum, v_sum = f1[mine], v1[...]
    for n in range(len(plane)):
        e_sum = e_sum + er1[n].astype(F32)
        l_sum = l_sum + lr1[n].astype(F32)
        f_sum = f_sum + fr1[n]
        v_sum = v_sum + vr1[n]
    e2[...] = e_sum.astype(BF)
    l2[...] = l_sum.astype(BF)
    f2[...] = f_sum
    v2[...] = v_sum
    stage2 = []
    for dz in range(1, s.z):
        to = (z + dz) % s.z
        peer = line_peer(dz)
        n = dz - 1
        stage2.append(remote(e2.at[to], er2.at[n], send2.at[0, n], recv2.at[0, n], peer))
        stage2.append(remote(l2.at[to], lr2.at[n], send2.at[1, n], recv2.at[1, n], peer))
        stage2.append(
            remote(
                f2.at[pl.ds(to * units, units)], fr2.at[n], send2.at[2, n], recv2.at[2, n], peer
            )
        )
        stage2.append(remote(v2, vr2.at[n], send2.at[3, n], recv2.at[3, n], peer))
    for copy in stage2:
        copy.start()
    for copy in copies:
        copy.wait()
    border = onehot(iota((s.node, s.hrows), 0) == out_rows[0:1, :])
    node_grad[...] = node_part[...] + dot(border, back[...])
    for copy in stage2:
        copy.wait()
    e_sum, l_sum = e2[z].astype(F32), l2[z].astype(F32)
    f_sum, v_sum = f2[pl.ds(z * units, units), :], v2[...]
    for n in range(s.z - 1):
        e_sum = e_sum + er2[n].astype(F32)
        l_sum = l_sum + lr2[n].astype(F32)
        f_sum = f_sum + fr2[n]
        v_sum = v_sum + vr2[n]
    early_out[...] = e_sum
    late_out[...] = l_sum
    vec_out[...] = v_sum
    for c in range(COARSE):
        for q in range(cuts):
            j = c * cuts + q
            span = slice(q * LANES, (q + 1) * LANES)
            node_grad[c : c + 1, span] += f_sum[j : j + 1, :]


def reduce_all(s, out_rows, need, node_part, ext_grad, early, late, vectors):
    width = node_part.shape[1]
    units = COARSE * width // LANES
    per_e, per_l = early.shape[1], late.shape[1]
    block = s.z * s.y
    planes = s.x * s.y
    full = pl.BlockSpec(memory_space=VMEM)
    sem = pltpu.SemaphoreType.DMA
    return pl.pallas_call(
        functools.partial(reduce_kernel, s),
        out_shape=[
            jax.ShapeDtypeStruct(node_part.shape, F32),
            jax.ShapeDtypeStruct((per_e, width), F32),
            jax.ShapeDtypeStruct((per_l, width), F32),
            jax.ShapeDtypeStruct(vectors.shape, F32),
        ],
        in_specs=[full] * 7,
        out_specs=[full] * 4,
        scratch_shapes=[
            VMEM((s.dev * units, LANES), F32),
            VMEM((s.hrows, width), BF),
            VMEM((s.x, block, per_e, width), BF),
            VMEM((s.x, block, per_l, width), BF),
            VMEM((s.x, block * units, LANES), F32),
            VMEM(vectors.shape, F32),
            VMEM((planes, s.z, per_e, width), BF),
            VMEM((planes, s.z, per_l, width), BF),
            VMEM((planes, s.z * units, LANES), F32),
            VMEM(vectors.shape, F32),
            VMEM((planes - 1, s.z, per_e, width), BF),
            VMEM((planes - 1, s.z, per_l, width), BF),
            VMEM((planes - 1, s.z * units, LANES), F32),
            VMEM((planes - 1,) + vectors.shape, F32),
            VMEM((s.z, per_e, width), BF),
            VMEM((s.z, per_l, width), BF),
            VMEM((s.z * units, LANES), F32),
            VMEM(vectors.shape, F32),
            VMEM((s.z - 1, per_e, width), BF),
            VMEM((s.z - 1, per_l, width), BF),
            VMEM((s.z - 1, units, LANES), F32),
            VMEM((s.z - 1,) + vectors.shape, F32),
            sem((4,)),
            sem((4,)),
            sem((4, s.x)),
            sem((4, s.x)),
            sem((4, planes - 1)),
            sem((4, planes - 1)),
            sem((4, s.z - 1)),
            sem((4, s.z - 1)),
        ],
        compiler_params=pltpu.CompilerParams(collective_id=1, has_side_effects=True),
        name="reduce",
    )(out_rows, need, node_part, ext_grad, early, late, vectors)


def shards(mesh, nodes, edges, senders, receivers, edge_count, halo_send, long_need, node_cot,
           edge_cot, e_w1, e_b1, e_w2, e_gain, n_w1, n_b1, n_w2, n_gain):
    nodes_l, edges_l = nodes[0, 0], edges[0, 0]
    node_n, width = nodes_l.shape
    edge_n = edges_l.shape[0]
    halo_n, slot_n = halo_send.shape[3], long_need.shape[3]
    s = Sizes(mesh, node_n, halo_n, slot_n)
    rows = jnp.pad(halo_send[0, 0], ((0, 0), (0, s.hslot - halo_n)), constant_values=-1)
    rows = rows.reshape(1, 4 * s.hslot)
    rows = jnp.pad(rows, ((0, 0), (0, s.hrows - 4 * s.hslot)), constant_values=-1)
    need = jnp.pad(
        long_need[0, 0].reshape(1, s.far_n), ((0, 0), (0, s.far - s.far_n)), constant_values=-1
    )
    ext = exchange_table(s, nodes_l, rows, need)
    weights = (e_w1, e_b1[None], e_w2, e_gain[None], n_w1, n_b1[None], n_w2, n_gain[None])
    ids = (edge_n // LANES, LANES)
    new_edges, edge_grad, new_nodes, node_part, ext_grad, early, late, vectors = layer(
        s, edge_count, senders.reshape(ids), receivers.reshape(ids), nodes_l, ext, edges_l,
        edge_cot[0, 0], node_cot[0, 0], weights,
    )
    late = late.reshape(s.dev, -1, width)
    node_grad, e_out, l_out, v_out = reduce_all(
        s, rows, need, node_part, ext_grad, early, late, vectors
    )
    me = lax.axis_index("lat") * s.lon + lax.axis_index("lon")
    part = width // s.dev
    vec = lax.dynamic_slice(v_out[:4], (0, me * part), (4, part))
    one, two = n_w1.shape[0] // s.dev, n_w2.shape[0] // s.dev
    return (
        new_nodes[None, None],
        new_edges[None, None],
        node_grad[None, None],
        edge_grad[None, None],
        l_out,
        vec[0],
        e_out[one + two :],
        vec[1],
        e_out[:one],
        vec[2],
        e_out[one : one + two],
        vec[3],
    )


def solution(mesh):
    grid4, grid3, both = P("lat", "lon", None, None), P("lat", "lon", None), P(("lat", "lon"))
    rows = P(("lat", "lon"), None)
    return jax.shard_map(
        functools.partial(shards, mesh),
        mesh=mesh,
        in_specs=(grid4, grid4, grid3, grid3, P("lat", "lon"), grid4, grid4, grid4, grid4)
        + (P(),) * 8,
        out_specs=(grid4,) * 4 + (rows, both) * 4,
        check_vma=False,
    )
```
